32 devices in a mesh: rep: 16 (over z, x, core), slab: 2 (over y).
Axes of the slice: x: 2, y: 2, z: 4, core: 2. Of those that a mesh axis runs over, the one named last changes fastest.
Arguments:
- weights: bfloat16 [16, 256, 3072], P('rep', 'slab'), may hold values from -6 to 6
- perms: int32 [16, 8, 256], P('rep'), may hold values from 0 to 255, each once within a row
Outputs:
- merged: bfloat16 [16, 256, 3072], P('rep', 'slab')
The draws below stay inside these ranges and needn't reach their ends.
Inputs may be any that keep to these rules, and one draw needn't show every extreme that they name: `perms`: each row of 256 entries names every neuron of the window once.
All inputs are finite; a program needn't handle non-finite values.
Results may differ from the reference program's by a relative error of at most 0.012.
Values may be sent and summed in bfloat16 or wider, within the bound.
A program may use at most 64 MiB of HBM per device.

```python
import math
import jax
import jax.numpy as jnp
from jax import lax

D = 3072
ROUNDS = 8
FFW = 256
REPLICAS = 16
N_REP = 16


def shard_levels(own_key, dims, cuts, smallest, top_value):
    loudness = 1.0
    for axis_at, parts in cuts:
        heights = jax.random.uniform(jax.random.fold_in(jax.random.fold_in(own_key, 6), axis_at), (parts,), jnp.float32, smallest / len(cuts), top_value / len(cuts))
        loudness = loudness * jnp.repeat(jnp.exp(heights), dims[axis_at] // parts).reshape((-1,) + (1,) * (len(dims) - 1 - axis_at))
    return loudness


def gaussian(own_key, shape, deviation, bound, split=(), kind=jnp.bfloat16):
    array = deviation * jax.random.normal(own_key, shape, jnp.float32)
    if split:
        array = array * shard_levels(own_key, shape, split, -0.22, 0.18)
    return jnp.clip(array, -bound, bound).astype(kind)


def setup_inputs(seed: int = 0) -> dict:
    arg_keys = jax.random.split(jax.random.key(seed), 3)
    weights = gaussian(arg_keys[0], (REPLICAS, FFW, D), 1.0, 6.0, ((0, 16), (1, 2)))
    perms = jax.vmap(lambda own: jax.random.permutation(own, FFW))(jax.random.split(arg_keys[1], REPLICAS * ROUNDS)).reshape((REPLICAS, ROUNDS, FFW)).astype(jnp.int32)
    return dict(weights=weights, perms=perms)


def merge_one(own, partner, perm_row):
    cost = jnp.dot(own, partner.T, preferred_element_type=jnp.float32) * (1.0 / math.sqrt(D))
    squared = cost * cost
    fourth = squared * squared
    soft_plan = fourth / (1.0 + lax.optimization_barrier(jnp.sum(fourth, axis=1, keepdims=True)))
    columns = jnp.arange(partner.shape[0], dtype=jnp.int32)
    onehot = (perm_row[:, None] == columns[None, :]).astype(jnp.float32)
    mixing = (onehot + soft_plan).astype(jnp.bfloat16)
    aligned = 0.5 * jnp.dot(mixing, partner, preferred_element_type=jnp.float32)
    return ((own.astype(jnp.float32) + aligned) * (1.0 / math.sqrt(2.0))).astype(jnp.bfloat16)

def reference(weights, perms):
    bit_count = N_REP.bit_length() - 1
    current = weights
    for round_idx in range(ROUNDS):
        flip = 1 << round_idx % bit_count
        partner_idx = jnp.bitwise_xor(jnp.arange(REPLICAS, dtype=jnp.int32), flip)
        partner = current[partner_idx]
        current = jax.vmap(merge_one)(current, partner, perms[:, round_idx])
    return current
```

```python
import functools
import math

import jax
import jax.numpy as jnp
from jax import lax
from jax.experimental import pallas as pl
from jax.experimental.pallas import tpu as pltpu
from jax.sharding import PartitionSpec as P

CHUNK = 256
PIECES = 4
LAG = 2


def kernel(n_rep, n_slab, rounds, cuts, w_ref, p_ref, out_ref,
           init, vis, sent, part, core_in, half_out, half_in, fourths, hot_v, hot_r, perms, rows_v, cols_v,
           in_send, in_recv, ex_send, ex_recv, core_send, core_recv, half_send, half_recv,
           out_send, home_send, out_recv, perm_send, perm_recv):
    bits = n_rep.bit_length() - 1
    me = lax.axis_index("rep")
    slab = lax.axis_index("slab")
    core = me % 2
    half, width = w_ref.shape[1], w_ref.shape[2]
    ffw = half * n_slab
    block = width // (2 * n_slab)
    scale = 1.0 / math.sqrt(width)

    def bit(b):
        return (me // (1 << b)) % 2

    def flipped(*at):
        to = me
        for b in at:
            to = to + (1 - 2 * bit(b)) * (1 << b)
        return to

    odd = sum(bit(b) for b in range(bits)) % 2
    resident = me + odd * (1 - 2 * core)

    def remote(src, dst, send, recv, rep_to, slab_to):
        return pltpu.make_async_remote_copy(
            src_ref=src, dst_ref=dst, send_sem=send, recv_sem=recv,
            device_id=(rep_to, slab_to), device_id_type=pl.DeviceIdType.MESH)

    barrier = pltpu.get_barrier_semaphore()
    devices = n_rep * n_slab

    def greet(k, carry):
        to = lax.rem(me * n_slab + slab + k, devices)
        pl.semaphore_signal(barrier, inc=1, device_id=(to // n_slab, to % n_slab),
                            device_id_type=pl.DeviceIdType.MESH)
        return carry

    lax.fori_loop(1, devices, greet, 0)
    pl.semaphore_wait(barrier, devices - 1)

    firsts = []
    rows_here = pl.ds(pl.multiple_of(slab * half, half), half)
    for ds_ in list(range(1, n_slab)) + [0]:
        for dc in range(2):
            slab_to = (slab + ds_) % n_slab
            core_to = core if dc == 0 else 1 - core
            start = (slab_to * 2 + core_to) * block
            src = w_ref.at[0, :, pl.ds(pl.multiple_of(start, 128), block)]
            dst = init.at[odd, rows_here]
            if ds_ == 0 and dc == 0:
                copy = pltpu.make_async_copy(src, dst, in_recv.at[0, 0])
            else:
                copy = remote(src, dst, in_send.at[ds_, dc], in_recv.at[ds_, dc],
                              me if dc == 0 else flipped(0), slab_to)
            copy.start()
            firsts.append(copy)

    perms[0] = p_ref[0]
    for b in range(bits):
        for c in range(2):
            if 2 * b + c > 0:
                to = flipped(b) if c == 0 else (flipped(0, b) if b else flipped(0))
                remote(p_ref.at[0], perms.at[2 * b + c], perm_send, perm_recv, to, slab).start()
    others = perms.at[pl.ds(1, 2 * bits - 1)]
    spread_all = remote(others, others, perm_send, perm_recv, flipped(0), slab)

    for copy in firsts:
        copy.wait()

    def visitor_of(r):
        return init.at[1] if r == 0 else vis.at[r - 1]

    def merged(own, mix, other):
        aligned = 0.5 * jnp.dot(mix, other, preferred_element_type=jnp.float32)
        return ((own.astype(jnp.float32) + aligned) * (1.0 / math.sqrt(2.0))).astype(jnp.bfloat16)

    chunks = [pl.ds(k * CHUNK, CHUNK) for k in range(block // CHUNK)]
    spans = [pl.ds(a, b - a) for a, b in zip(cuts[:-1], cuts[1:])]
    columns = lax.broadcasted_iota(jnp.int32, (ffw, ffw), 1)
    rows = lax.broadcasted_iota(jnp.int32, (ffw, ffw), 0)

    def hots(r):
        hot_v[...] = (cols_v[:, r:r + 1].astype(jnp.int32) == columns).astype(jnp.float32)
        hot_r[...] = (perms[odd, r:r + 1, :] == rows).astype(jnp.float32)

    pending = []
    arrivals = None
    source = slab * 2 + core
    for r in range(rounds):
        last = r == rounds - 1
        visitor = visitor_of(r)
        sums = [[] for _ in spans]
        total_columns = [None]
        onward = []

        def cost(q):
            its = spans[q]
            if r:
                arrivals[q].wait_recv()
            partial = lax.dot_general(visitor[its, :], init[0], (((1,), (1,)), ((), ())),
                                      preferred_element_type=jnp.float32)
            part[r, its, :] = partial
            half_out[r, its, :] = partial.astype(half_out.dtype)
            for ds_ in range(1, n_slab):
                for dc in range(2):
                    at = 2 * (ds_ - 1) + dc
                    sums[q].append(remote(half_out.at[r, its], half_in.at[r, at, its], half_send.at[r, at, q],
                                          half_recv.at[r, at, q], me if dc == 0 else flipped(0),
                                          (slab + ds_) % n_slab))
            sums[q].append(remote(part.at[r, its], core_in.at[r, its], core_send.at[r, q], core_recv.at[r, q],
                                  flipped(0), slab))
            for copy in sums[q]:
                copy.start()

        def finish(q):
            its = spans[q]
            for copy in sums[q]:
                copy.wait_recv()
            total = part[r, its, :] + core_in[r, its, :]
            for at in range(2 * (n_slab - 1)):
                total = total + half_in[r, at, its, :].astype(jnp.float32)
            scaled = total * scale
            squared = scaled * scaled
            fourth = squared * squared
            fourths[its, :] = fourth
            by_row = 1.0 / (1.0 + jnp.sum(fourth, axis=1, keepdims=True))
            mix = (hot_v[its, :] + fourth * by_row).astype(jnp.bfloat16)
            for k in chunks:
                sent[r, its, k] = merged(visitor[its, k], mix, init[0, :, k])
            if last:
                h = cuts[q] // half
                dst = out_ref.at[0, pl.ds(cuts[q] - h * half, cuts[q + 1] - cuts[q]),
                                 pl.ds(pl.multiple_of(source * block, 128), block)]
                j = resident_flipped(r % bits)
                copy = remote(sent.at[r, its], dst, out_send.at[q], out_recv.at[source], j, h)
            else:
                copy = remote(sent.at[r, its], vis.at[r, its], ex_send.at[r, q], ex_recv.at[r, q],
                              flipped(*[b for b in (r % bits, (r + 1) % bits) if b]), slab)
            copy.start()
            onward.append(copy)
            by_columns = jnp.sum(fourth, axis=0, keepdims=True)
            total_columns[0] = by_columns if total_columns[0] is None else total_columns[0] + by_columns

        def resident_flipped(b):
            if b == 0:
                return me + (1 - odd) * (1 - 2 * core)
            return resident + (1 - 2 * bit(b)) * (1 << b)

        lag = len(spans) if r == 0 else LAG
        for q in range(len(spans) + lag):
            if q < len(spans):
                cost(q)
            if r == 0 and q == len(spans) - 1:
                spread_all.wait()
                for s in range(rounds):
                    b = s % bits
                    rows_v[s:s + 1, :] = (perms[2 * b + odd, s:s + 1, :] if b else
                                          perms[1 - odd, s:s + 1, :]).astype(jnp.float32)
                cols_v[...] = rows_v[...].T
                hots(0)
            if q >= lag:
                finish(q - lag)

        by_column = 1.0 / (1.0 + total_columns[0])
        mix = (hot_r[...] + fourths[...] * by_column).astype(jnp.bfloat16).T
        for k in chunks:
            init[0, :, k] = merged(init[0, :, k], mix, visitor[:, k])
        pending += sum(sums, [])
        arrivals = onward
        if last:
            for h in range(n_slab):
                src = init.at[0, pl.ds(h * half, half)]
                dst = out_ref.at[0, :, pl.ds(pl.multiple_of(source * block, 128), block)]
                stay = jnp.logical_and(odd == 0, slab == h)

                @pl.when(stay)
                def _():
                    pltpu.make_async_copy(src, dst, out_recv.at[source]).start()

                @pl.when(jnp.logical_not(stay))
                def _():
                    remote(src, dst, home_send.at[h], out_recv.at[source], resident, h).start()
            for copy in onward:
                copy.wait_send()
            for h in range(n_slab):
                stay = jnp.logical_and(odd == 0, slab == h)

                @pl.when(jnp.logical_not(stay))
                def _():
                    src = init.at[0, pl.ds(h * half, half)]
                    dst = out_ref.at[0, :, pl.ds(0, block)]
                    remote(src, dst, home_send.at[h], out_recv.at[0], resident, h).wait_send()
            for s in range(2 * n_slab):
                dst = out_ref.at[0, :, pl.ds(s * block, block)]
                pltpu.make_async_copy(dst, dst, out_recv.at[s]).wait()
        else:
            pending += onward
            hots(r + 1)
    for copy in pending:
        copy.wait_send()


def solution(mesh):
    n_rep, n_slab = mesh.shape["rep"], mesh.shape["slab"]

    def local(weights, perms):
        _, half, width = weights.shape
        rounds = perms.shape[1]
        ffw = perms.shape[2]
        bits = n_rep.bit_length() - 1
        block = width // (2 * n_slab)
        size = ffw // PIECES
        cuts = list(range(0, ffw + 1, size))
        pieces = len(cuts) - 1
        vmem = pltpu.VMEM
        dma = pltpu.SemaphoreType.DMA
        bf16, f32 = jnp.bfloat16, jnp.float32
        away = 2 * (n_slab - 1)
        return pl.pallas_call(
            functools.partial(kernel, n_rep, n_slab, rounds, cuts),
            out_shape=jax.ShapeDtypeStruct(weights.shape, weights.dtype),
            in_specs=[pl.BlockSpec(memory_space=pltpu.VMEM)] * 2,
            out_specs=pl.BlockSpec(memory_space=pltpu.VMEM),
            scratch_shapes=[
                vmem((2, ffw, block), bf16),
                vmem((rounds - 1, ffw, block), bf16),
                vmem((rounds, ffw, block), bf16),
                vmem((rounds, ffw, ffw), f32),
                vmem((rounds, ffw, ffw), f32),
                vmem((rounds, ffw, ffw), bf16),
                vmem((rounds, away, ffw, ffw), bf16),
                vmem((ffw, ffw), f32),
                vmem((ffw, ffw), f32),
                vmem((ffw, ffw), f32),
                vmem((2 * bits, rounds, ffw), jnp.int32),
                vmem((rounds, ffw), f32),
                vmem((ffw, rounds), f32),
                dma((n_slab, 2)), dma((n_slab, 2)),
                dma((rounds, pieces)), dma((rounds, pieces)),
                dma((rounds, pieces)), dma((rounds, pieces)),
                dma((rounds, away, pieces)), dma((rounds, away, pieces)),
                dma((pieces,)), dma((n_slab,)), dma((2 * n_slab,)),
                dma, dma,
            ],
            compiler_params=pltpu.CompilerParams(collective_id=0, has_side_effects=True, vmem_limit_bytes=60 * 1024 * 1024),
        )(weights, perms)

    return jax.shard_map(
        local, mesh=mesh, in_specs=(P("rep", "slab", None), P("rep", None, None)),
        out_specs=P("rep", "slab", None), check_vma=False,
    )
```

```python
import functools
import math

import jax
import jax.numpy as jnp
from jax import lax
from jax.experimental import pallas as pl
from jax.experimental.pallas import tpu as pltpu
from jax.sharding import PartitionSpec as P

CHUNK = 256
PIECES = 4
LAG = 2


def moves(r, bits):
    return tuple(sorted(b for b in ((r - 1) % bits, r % bits) if b))


def kernel(n_rep, n_slab, rounds, cuts, w_hbm, p_hbm, out_ref,
           w_ref, p_ref, init, vis, sent, part, core_in, half_out, half_in, fourths, hot_v, hot_r, perms, rows_v, cols_v,
           load, in_send, in_recv, ex_send, ex_recv, core_send, core_recv, half_send, half_recv,
           out_send, home_send, out_recv, perm_send, perm_recv):
    bits = n_rep.bit_length() - 1
    me = lax.axis_index("rep")
    slab = lax.axis_index("slab")
    core = me % 2
    half, width = w_ref.shape[1], w_ref.shape[2]
    ffw = half * n_slab
    block = width // (2 * n_slab)
    scale = 1.0 / math.sqrt(width)

    def bit(b):
        return (me // (1 << b)) % 2

    def flipped(*at):
        to = me
        for b in at:
            to = to + (1 - 2 * bit(b)) * (1 << b)
        return to

    odd = sum(bit(b) for b in range(bits)) % 2
    resident = me + odd * (1 - 2 * core)

    def remote(src, dst, send, recv, rep_to, slab_to):
        return pltpu.make_async_remote_copy(
            src_ref=src, dst_ref=dst, send_sem=send, recv_sem=recv,
            device_id=(rep_to, slab_to), device_id_type=pl.DeviceIdType.MESH)

    loads = [pltpu.make_async_copy(p_hbm, p_ref, load.at[0]), pltpu.make_async_copy(w_hbm, w_ref, load.at[1])]
    for copy in loads:
        copy.start()

    near = {(0,)} | {tuple(sorted({0, b} - {0} | extra)) for b in range(1, bits) for extra in ({0}, set())}
    for r in range(1, rounds):
        near.add(moves(r, bits))
    final = (rounds - 1) % bits
    across = {(), (0,), tuple({final} - {0}), tuple(sorted({0, final}))}
    peers = [(at, 0) for at in sorted(near | across) if at]
    peers += [(at, ds_) for ds_ in range(1, n_slab) for at in sorted(across)]
    barrier = pltpu.get_barrier_semaphore()
    for at, ds_ in peers:
        pl.semaphore_signal(barrier, inc=1, device_id=(flipped(*at), (slab + ds_) % n_slab),
                            device_id_type=pl.DeviceIdType.MESH)
    pl.semaphore_wait(barrier, len(peers))
    for copy in loads:
        copy.wait()

    firsts = []
    rows_here = pl.ds(pl.multiple_of(slab * half, half), half)
    for ds_ in list(range(1, n_slab)) + [0]:
        for dc in range(2):
            slab_to = (slab + ds_) % n_slab
            core_to = core if dc == 0 else 1 - core
            start = (slab_to * 2 + core_to) * block
            src = w_ref.at[0, :, pl.ds(pl.multiple_of(start, 128), block)]
            dst = init.at[odd, rows_here]
            if ds_ == 0 and dc == 0:
                copy = pltpu.make_async_copy(src, dst, in_recv.at[0, 0])
            else:
                copy = remote(src, dst, in_send.at[ds_, dc], in_recv.at[ds_, dc],
                              me if dc == 0 else flipped(0), slab_to)
            copy.start()
            firsts.append(copy)

    perms[0] = p_ref[0]
    for b in range(bits):
        for c in range(2):
            if 2 * b + c > 0:
                to = flipped(b) if c == 0 else (flipped(0, b) if b else flipped(0))
                remote(p_ref.at[0], perms.at[2 * b + c], perm_send, perm_recv, to, slab).start()
    others = perms.at[pl.ds(1, 2 * bits - 1)]
    spread_all = remote(others, others, perm_send, perm_recv, flipped(0), slab)

    def visitor_of(r):
        return init.at[1] if r == 0 else vis.at[r - 1]

    def merged(own, mix, other):
        aligned = 0.5 * jnp.dot(mix, other, preferred_element_type=jnp.float32)
        return ((own.astype(jnp.float32) + aligned) * (1.0 / math.sqrt(2.0))).astype(jnp.bfloat16)

    chunks = [pl.ds(k * CHUNK, CHUNK) for k in range(block // CHUNK)]
    spans = [pl.ds(a, b - a) for a, b in zip(cuts[:-1], cuts[1:])]
    columns = lax.broadcasted_iota(jnp.int32, (ffw, ffw), 1)
    rows = lax.broadcasted_iota(jnp.int32, (ffw, ffw), 0)

    spread_all.wait()
    for r in range(rounds):
        b = r % bits
        rows_v[r:r + 1, :] = (perms[2 * b + odd, r:r + 1, :] if b else perms[1 - odd, r:r + 1, :]).astype(jnp.float32)
    cols_v[...] = rows_v[...].T
    for r in range(rounds):
        hot_v[r] = (cols_v[:, r:r + 1].astype(jnp.int32) == columns).astype(jnp.float32)
        hot_r[r] = (perms[odd, r:r + 1, :] == rows).astype(jnp.float32)
    for copy in firsts:
        copy.wait()

    pending = []
    arrivals = None
    source = slab * 2 + core
    for r in range(rounds):
        last = r == rounds - 1
        visitor = visitor_of(r)
        sums = [[] for _ in spans]
        total_columns = [None]
        onward = []

        def cost(q):
            its = spans[q]
            if r:
                arrivals[q].wait_recv()
            partial = lax.dot_general(visitor[its, :], init[0], (((1,), (1,)), ((), ())),
                                      preferred_element_type=jnp.float32)
            part[r, its, :] = partial
            half_out[r, its, :] = partial.astype(half_out.dtype)
            for ds_ in range(1, n_slab):
                for dc in range(2):
                    at = 2 * (ds_ - 1) + dc
                    sums[q].append(remote(half_out.at[r, its], half_in.at[r, at, its], half_send.at[r, at, q],
                                          half_recv.at[r, at, q], me if dc == 0 else flipped(0),
                                          (slab + ds_) % n_slab))
            sums[q].append(remote(part.at[r, its], core_in.at[r, its], core_send.at[r, q], core_recv.at[r, q],
                                  flipped(0), slab))
            for copy in sums[q]:
                copy.start()

        def finish(q):
            its = spans[q]
            for copy in sums[q]:
                copy.wait_recv()
            total = part[r, its, :] + core_in[r, its, :]
            for at in range(2 * (n_slab - 1)):
                total = total + half_in[r, at, its, :].astype(jnp.float32)
            scaled = total * scale
            squared = scaled * scaled
            fourth = squared * squared
            fourths[its, :] = fourth
            by_row = 1.0 / (1.0 + jnp.sum(fourth, axis=1, keepdims=True))
            mix = (hot_v[r, its, :] + fourth * by_row).astype(jnp.bfloat16)
            for k in chunks:
                sent[r, its, k] = merged(visitor[its, k], mix, init[0, :, k])
            if last:
                h = cuts[q] // half
                dst = out_ref.at[0, pl.ds(cuts[q] - h * half, cuts[q + 1] - cuts[q]),
                                 pl.ds(pl.multiple_of(source * block, 128), block)]
                j = resident_flipped(r % bits)
                copy = remote(sent.at[r, its], dst, out_send.at[q], out_recv.at[source], j, h)
            else:
                copy = remote(sent.at[r, its], vis.at[r, its], ex_send.at[r, q], ex_recv.at[r, q],
                              flipped(*moves(r + 1, bits)), slab)
            copy.start()
            onward.append(copy)
            by_columns = jnp.sum(fourth, axis=0, keepdims=True)
            total_columns[0] = by_columns if total_columns[0] is None else total_columns[0] + by_columns

        def resident_flipped(b):
            if b == 0:
                return me + (1 - odd) * (1 - 2 * core)
            return resident + (1 - 2 * bit(b)) * (1 << b)

        lag = len(spans) if r == 0 else 1 if bits - 1 in moves(r, bits) else LAG
        for q in range(len(spans) + lag):
            if q < len(spans):
                cost(q)
            if q >= lag:
                finish(q - lag)

        by_column = 1.0 / (1.0 + total_columns[0])
        mix = (hot_r[r] + fourths[...] * by_column).astype(jnp.bfloat16).T
        for k in chunks:
            init[0, :, k] = merged(init[0, :, k], mix, visitor[:, k])
        pending += sum(sums, [])
        arrivals = onward
        if last:
            for h in range(n_slab):
                src = init.at[0, pl.ds(h * half, half)]
                dst = out_ref.at[0, :, pl.ds(pl.multiple_of(source * block, 128), block)]
                stay = jnp.logical_and(odd == 0, slab == h)

                @pl.when(stay)
                def _():
                    pltpu.make_async_copy(src, dst, out_recv.at[source]).start()

                @pl.when(jnp.logical_not(stay))
                def _():
                    remote(src, dst, home_send.at[h], out_recv.at[source], resident, h).start()
            for copy in onward:
                copy.wait_send()
            for h in range(n_slab):
                stay = jnp.logical_and(odd == 0, slab == h)

                @pl.when(jnp.logical_not(stay))
                def _():
                    src = init.at[0, pl.ds(h * half, half)]
                    dst = out_ref.at[0, :, pl.ds(0, block)]
                    remote(src, dst, home_send.at[h], out_recv.at[0], resident, h).wait_send()
            for s in range(2 * n_slab):
                dst = out_ref.at[0, :, pl.ds(s * block, block)]
                pltpu.make_async_copy(dst, dst, out_recv.at[s]).wait()
        else:
            pending += onward
    for copy in pending:
        copy.wait_send()


def solution(mesh):
    n_rep, n_slab = mesh.shape["rep"], mesh.shape["slab"]

    def local(weights, perms):
        _, half, width = weights.shape
        rounds = perms.shape[1]
        ffw = perms.shape[2]
        bits = n_rep.bit_length() - 1
        block = width // (2 * n_slab)
        size = ffw // PIECES
        cuts = list(range(0, ffw + 1, size))
        pieces = len(cuts) - 1
        vmem = pltpu.VMEM
        dma = pltpu.SemaphoreType.DMA
        bf16, f32 = jnp.bfloat16, jnp.float32
        away = 2 * (n_slab - 1)
        return pl.pallas_call(
            functools.partial(kernel, n_rep, n_slab, rounds, cuts),
            out_shape=pltpu.VMEM(weights.shape, weights.dtype),
            in_specs=[pl.BlockSpec(memory_space=pl.ANY)] * 2,
            out_specs=pl.BlockSpec(memory_space=pltpu.VMEM),
            scratch_shapes=[
                vmem(weights.shape, bf16), vmem(perms.shape, jnp.int32),
                vmem((2, ffw, block), bf16),
                vmem((rounds - 1, ffw, block), bf16),
                vmem((rounds, ffw, block), bf16),
                vmem((rounds, ffw, ffw), f32),
                vmem((rounds, ffw, ffw), f32),
                vmem((rounds, ffw, ffw), bf16),
                vmem((rounds, away, ffw, ffw), bf16),
                vmem((ffw, ffw), f32),
                vmem((rounds, ffw, ffw), f32),
                vmem((rounds, ffw, ffw), f32),
                vmem((2 * bits, rounds, ffw), jnp.int32),
                vmem((rounds, ffw), f32),
                vmem((ffw, rounds), f32),
                dma((2,)), dma((n_slab, 2)), dma((n_slab, 2)),
                dma((rounds, pieces)), dma((rounds, pieces)),
                dma((rounds, pieces)), dma((rounds, pieces)),
                dma((rounds, away, pieces)), dma((rounds, away, pieces)),
                dma((pieces,)), dma((n_slab,)), dma((2 * n_slab,)),
                dma, dma,
            ],
            compiler_params=pltpu.CompilerParams(collective_id=0, has_side_effects=True, vmem_limit_bytes=60 * 1024 * 1024),
        )(weights, perms)

    return jax.shard_map(
        local, mesh=mesh, in_specs=(P("rep", "slab", None), P("rep", None, None)),
        out_specs=P("rep", "slab", None), check_vma=False,
    )
```

```python
import functools
import math

import jax
import jax.numpy as jnp
from jax import lax
from jax.experimental import pallas as pl
from jax.experimental.pallas import tpu as pltpu
from jax.sharding import PartitionSpec as P

CHUNK = 256
PARTS = 2
LAG = 2


def moves(r, bits):
    return tuple(sorted(b for b in ((r - 1) % bits, r % bits) if b))


def kernel(n_rep, n_slab, rounds, parts, w_hbm, p_hbm, out_ref,
           w_ref, p_ref, stage, init, vis, sent, part, core_in, half_out, half_in, fourths, hot_v, hot_r, perms, rows_v, cols_v,
           load, give_send, give_recv, still_send, still_recv, first_send, first_recv, in_send, in_recv, ex_send, ex_recv, core_send, core_recv, half_send, half_recv,
           out_send, home_send, out_recv, perm_send, perm_recv):
    bits = n_rep.bit_length() - 1
    me = lax.axis_index("rep")
    slab = lax.axis_index("slab")
    core = me % 2
    half, width = w_ref.shape[1], w_ref.shape[2]
    ffw = half * n_slab
    block = width // (2 * n_slab)
    scale = 1.0 / math.sqrt(width)

    def bit(b):
        return (me // (1 << b)) % 2

    def flipped(*at):
        to = me
        for b in at:
            to = to + (1 - 2 * bit(b)) * (1 << b)
        return to

    odd = sum(bit(b) for b in range(bits)) % 2
    resident = me + odd * (1 - 2 * core)

    def remote(src, dst, send, recv, rep_to, slab_to):
        return pltpu.make_async_remote_copy(
            src_ref=src, dst_ref=dst, send_sem=send, recv_sem=recv,
            device_id=(rep_to, slab_to), device_id_type=pl.DeviceIdType.MESH)

    loads = [pltpu.make_async_copy(p_hbm, p_ref, load.at[0]), pltpu.make_async_copy(w_hbm, w_ref, load.at[1])]
    for copy in loads:
        copy.start()

    near = {(0,)} | {tuple(sorted({0, b} - {0} | extra)) for b in range(1, bits) for extra in ({0}, set())}
    for r in range(1, rounds):
        near.add(moves(r, bits))
    final = (rounds - 1) % bits
    across = {(), (0,), tuple({final} - {0}), tuple(sorted({0, final}))}
    peers = [(at, 0) for at in sorted(near | across) if at]
    peers += [(at, ds_) for ds_ in range(1, n_slab) for at in sorted(across)]
    barrier = pltpu.get_barrier_semaphore()
    for at, ds_ in peers:
        pl.semaphore_signal(barrier, inc=1, device_id=(flipped(*at), (slab + ds_) % n_slab),
                            device_id_type=pl.DeviceIdType.MESH)
    pl.semaphore_wait(barrier, len(peers))
    for copy in loads:
        copy.wait()

    def columns_of(slab_at, core_at):
        return pl.ds(pl.multiple_of((slab_at * 2 + core_at) * block, 128), block)

    base = slab * half
    rows_here = pl.ds(pl.multiple_of(base, half), half)
    gives, stills, moved = [], [], [[] for _ in parts[1:]]
    for ds_ in range(1, n_slab):
        gives.append(remote(w_ref.at[0, :, columns_of((slab + ds_) % n_slab, 1 - core)], stage.at[ds_ - 1],
                            give_send.at[ds_ - 1], give_recv.at[ds_ - 1], flipped(0), slab))
        gives[-1].start()
    own = pltpu.make_async_copy(w_ref.at[0, :, columns_of(slab, core)], init.at[odd, rows_here], first_recv.at[0])
    beside = remote(w_ref.at[0, :, columns_of(slab, 1 - core)], init.at[odd, rows_here], first_send,
                    first_recv.at[1], flipped(0), slab)

    def crossing(ds_, src, kind, k):
        slab_to = (slab + ds_) % n_slab
        if kind == 0:
            return remote(src, init.at[0, rows_here], still_send.at[ds_ - 1], still_recv.at[ds_ - 1], me, slab_to)
        size = parts[k + 1] - parts[k]
        dst = init.at[1, pl.ds(pl.multiple_of(base + parts[k], 16), size)]
        return remote(src.at[pl.ds(parts[k], size)], dst, in_send.at[ds_ - 1, k], in_recv.at[ds_ - 1, k], me, slab_to)

    def mine(ds_):
        return w_ref.at[0, :, columns_of((slab + ds_) % n_slab, core)]

    @pl.when(odd == 0)
    def _():
        for ds_ in range(1, n_slab):
            crossing(ds_, mine(ds_), 0, 0).start()

    own.start()
    beside.start()
    for copy in gives:
        copy.wait_recv()

    @pl.when(odd == 0)
    def _():
        for k in range(len(parts) - 1):
            for ds_ in range(1, n_slab):
                crossing(ds_, stage.at[ds_ - 1], 1, k).start()

    @pl.when(odd == 1)
    def _():
        for ds_ in range(1, n_slab):
            crossing(ds_, stage.at[ds_ - 1], 0, 0).start()
        for k in range(len(parts) - 1):
            for ds_ in range(1, n_slab):
                crossing(ds_, mine(ds_), 1, k).start()

    for ds_ in range(1, n_slab):
        stills.append(crossing(ds_, stage.at[ds_ - 1], 0, 0))
        for k in range(len(parts) - 1):
            moved[k].append(crossing(ds_, stage.at[ds_ - 1], 1, k))

    perms[0] = p_ref[0]
    for b in range(bits):
        for c in range(2):
            if 2 * b + c > 0:
                to = flipped(b) if c == 0 else (flipped(0, b) if b else flipped(0))
                remote(p_ref.at[0], perms.at[2 * b + c], perm_send, perm_recv, to, slab).start()
    others = perms.at[pl.ds(1, 2 * bits - 1)]
    spread_all = remote(others, others, perm_send, perm_recv, flipped(0), slab)

    def visitor_of(r):
        return init.at[1] if r == 0 else vis.at[r - 1]

    def merged(own, mix, other):
        aligned = 0.5 * jnp.dot(mix, other, preferred_element_type=jnp.float32)
        return ((own.astype(jnp.float32) + aligned) * (1.0 / math.sqrt(2.0))).astype(jnp.bfloat16)

    chunks = [pl.ds(k * CHUNK, CHUNK) for k in range(block // CHUNK)]
    cuts = [(h * half + a, h * half + b) for a, b in zip(parts[:-1], parts[1:]) for h in range(n_slab)]
    spans = [pl.ds(a, b - a) for a, b in cuts]
    columns = lax.broadcasted_iota(jnp.int32, (ffw, ffw), 1)
    rows = lax.broadcasted_iota(jnp.int32, (ffw, ffw), 0)

    spread_all.wait()
    for r in range(rounds):
        b = r % bits
        rows_v[r:r + 1, :] = (perms[2 * b + odd, r:r + 1, :] if b else perms[1 - odd, r:r + 1, :]).astype(jnp.float32)
    cols_v[...] = rows_v[...].T
    for r in range(rounds):
        hot_v[r] = (cols_v[:, r:r + 1].astype(jnp.int32) == columns).astype(jnp.float32)
        hot_r[r] = (perms[odd, r:r + 1, :] == rows).astype(jnp.float32)
    own.wait()
    beside.wait_recv()
    for copy in stills:
        copy.wait_recv()

    pending = gives + [beside] + stills + sum(moved, [])
    arrivals = None
    source = slab * 2 + core
    for r in range(rounds):
        last = r == rounds - 1
        visitor = visitor_of(r)
        sums = [[] for _ in spans]
        total_columns = [None]
        onward = []

        def cost(q):
            its = spans[q]
            if r:
                arrivals[q].wait_recv()
            elif q % n_slab == 0:
                for copy in moved[q // n_slab]:
                    copy.wait_recv()
            partial = lax.dot_general(visitor[its, :], init[0], (((1,), (1,)), ((), ())),
                                      preferred_element_type=jnp.float32)
            part[r, its, :] = partial
            half_out[r, its, :] = partial.astype(half_out.dtype)
            for ds_ in range(1, n_slab):
                for dc in range(2):
                    at = 2 * (ds_ - 1) + dc
                    sums[q].append(remote(half_out.at[r, its], half_in.at[r, at, its], half_send.at[r, at, q],
                                          half_recv.at[r, at, q], me if dc == 0 else flipped(0),
                                          (slab + ds_) % n_slab))
            sums[q].append(remote(part.at[r, its], core_in.at[r, its], core_send.at[r, q], core_recv.at[r, q],
                                  flipped(0), slab))
            for copy in sums[q]:
                copy.start()

        def finish(q):
            its = spans[q]
            for copy in sums[q]:
                copy.wait_recv()
            total = part[r, its, :] + core_in[r, its, :]
            for at in range(2 * (n_slab - 1)):
                total = total + half_in[r, at, its, :].astype(jnp.float32)
            scaled = total * scale
            squared = scaled * scaled
            fourth = squared * squared
            fourths[its, :] = fourth
            by_row = 1.0 / (1.0 + jnp.sum(fourth, axis=1, keepdims=True))
            mix = (hot_v[r, its, :] + fourth * by_row).astype(jnp.bfloat16)
            for k in chunks:
                sent[r, its, k] = merged(visitor[its, k], mix, init[0, :, k])
            if last:
                h = cuts[q][0] // half
                dst = out_ref.at[0, pl.ds(cuts[q][0] - h * half, cuts[q][1] - cuts[q][0]),
                                 pl.ds(pl.multiple_of(source * block, 128), block)]
                j = resident_flipped(r % bits)
                copy = remote(sent.at[r, its], dst, out_send.at[q], out_recv.at[source], j, h)
            else:
                copy = remote(sent.at[r, its], vis.at[r, its], ex_send.at[r, q], ex_recv.at[r, q],
                              flipped(*moves(r + 1, bits)), slab)
            copy.start()
            onward.append(copy)
            by_columns = jnp.sum(fourth, axis=0, keepdims=True)
            total_columns[0] = by_columns if total_columns[0] is None else total_columns[0] + by_columns

        def resident_flipped(b):
            if b == 0:
                return me + (1 - odd) * (1 - 2 * core)
            return resident + (1 - 2 * bit(b)) * (1 << b)

        lag = len(spans) if r == 0 else 1 if bits - 1 in moves(r, bits) else LAG
        for q in range(len(spans) + lag):
            if q < len(spans):
                cost(q)
            if q >= lag:
                finish(q - lag)

        by_column = 1.0 / (1.0 + total_columns[0])
        mix = (hot_r[r] + fourths[...] * by_column).astype(jnp.bfloat16).T
        for k in chunks:
            init[0, :, k] = merged(init[0, :, k], mix, visitor[:, k])
        pending += sum(sums, [])
        arrivals = onward
        if last:
            for h in range(n_slab):
                src = init.at[0, pl.ds(h * half, half)]
                dst = out_ref.at[0, :, pl.ds(pl.multiple_of(source * block, 128), block)]
                stay = jnp.logical_and(odd == 0, slab == h)

                @pl.when(stay)
                def _():
                    pltpu.make_async_copy(src, dst, out_recv.at[source]).start()

                @pl.when(jnp.logical_not(stay))
                def _():
                    remote(src, dst, home_send.at[h], out_recv.at[source], resident, h).start()
            for copy in onward:
                copy.wait_send()
            for h in range(n_slab):
                stay = jnp.logical_and(odd == 0, slab == h)

                @pl.when(jnp.logical_not(stay))
                def _():
                    src = init.at[0, pl.ds(h * half, half)]
                    dst = out_ref.at[0, :, pl.ds(0, block)]
                    remote(src, dst, home_send.at[h], out_recv.at[0], resident, h).wait_send()
            for s in range(2 * n_slab):
                dst = out_ref.at[0, :, pl.ds(s * block, block)]
                pltpu.make_async_copy(dst, dst, out_recv.at[s]).wait()
        else:
            pending += onward
    for copy in pending:
        copy.wait_send()


def solution(mesh):
    n_rep, n_slab = mesh.shape["rep"], mesh.shape["slab"]

    def local(weights, perms):
        _, half, width = weights.shape
        rounds = perms.shape[1]
        ffw = perms.shape[2]
        bits = n_rep.bit_length() - 1
        block = width // (2 * n_slab)
        parts = [k * half // PARTS for k in range(PARTS + 1)]
        pieces = PARTS * n_slab
        vmem = pltpu.VMEM
        dma = pltpu.SemaphoreType.DMA
        bf16, f32 = jnp.bfloat16, jnp.float32
        away = 2 * (n_slab - 1)
        return pl.pallas_call(
            functools.partial(kernel, n_rep, n_slab, rounds, parts),
            out_shape=pltpu.VMEM(weights.shape, weights.dtype),
            in_specs=[pl.BlockSpec(memory_space=pl.ANY)] * 2,
            out_specs=pl.BlockSpec(memory_space=pltpu.VMEM),
            scratch_shapes=[
                vmem(weights.shape, bf16), vmem(perms.shape, jnp.int32),
                vmem((n_slab - 1, half, block), bf16),
                vmem((2, ffw, block), bf16),
                vmem((rounds - 1, ffw, block), bf16),
                vmem((rounds, ffw, block), bf16),
                vmem((rounds, ffw, ffw), f32),
                vmem((rounds, ffw, ffw), f32),
                vmem((rounds, ffw, ffw), bf16),
                vmem((rounds, away, ffw, ffw), bf16),
                vmem((ffw, ffw), f32),
                vmem((rounds, ffw, ffw), f32),
                vmem((rounds, ffw, ffw), f32),
                vmem((2 * bits, rounds, ffw), jnp.int32),
                vmem((rounds, ffw), f32),
                vmem((ffw, rounds), f32),
                dma((2,)), dma((n_slab - 1,)), dma((n_slab - 1,)), dma((n_slab - 1,)), dma((n_slab - 1,)),
                dma, dma((2,)), dma((n_slab - 1, PARTS)), dma((n_slab - 1, PARTS)),
                dma((rounds, pieces)), dma((rounds, pieces)),
                dma((rounds, pieces)), dma((rounds, pieces)),
                dma((rounds, away, pieces)), dma((rounds, away, pieces)),
                dma((pieces,)), dma((n_slab,)), dma((2 * n_slab,)),
                dma, dma,
            ],
            compiler_params=pltpu.CompilerParams(collective_id=0, has_side_effects=True, vmem_limit_bytes=60 * 1024 * 1024),
        )(weights, perms)

    return jax.shard_map(
        local, mesh=mesh, in_specs=(P("rep", "slab", None), P("rep", None, None)),
        out_specs=P("rep", "slab", None), check_vma=False,
    )
```

```python
import functools
import math

import jax
import jax.numpy as jnp
from jax import lax
from jax.experimental import pallas as pl
from jax.experimental.pallas import tpu as pltpu
from jax.sharding import PartitionSpec as P

CHUNK = 256
PARTS = 2
LAG = 2


def moves(r, bits):
    return tuple(sorted(b for b in ((r - 1) % bits, r % bits) if b))


def kernel(n_rep, n_slab, rounds, parts, w_hbm, p_hbm, out_ref,
           w_ref, p_ref, stage, init, vis, sent, part, core_in, half_out, half_in, fourths, hot_v, hot_r, perms, rows_v, cols_v,
           load, give_send, give_recv, still_send, still_recv, first_send, first_recv, in_send, in_recv, ex_send, ex_recv, core_send, core_recv, half_send, half_recv,
           out_send, home_send, out_recv, perm_send, perm_recv):
    bits = n_rep.bit_length() - 1
    me = lax.axis_index("rep")
    slab = lax.axis_index("slab")
    core = me % 2
    half, width = w_ref.shape[1], w_ref.shape[2]
    ffw = half * n_slab
    block = width // (2 * n_slab)
    scale = 1.0 / math.sqrt(width)

    def bit(b):
        return (me // (1 << b)) % 2

    def flipped(*at):
        to = me
        for b in at:
            to = to + (1 - 2 * bit(b)) * (1 << b)
        return to

    odd = sum(bit(b) for b in range(bits)) % 2
    resident = me + odd * (1 - 2 * core)

    def remote(src, dst, send, recv, rep_to, slab_to):
        return pltpu.make_async_remote_copy(
            src_ref=src, dst_ref=dst, send_sem=send, recv_sem=recv,
            device_id=(rep_to, slab_to), device_id_type=pl.DeviceIdType.MESH)

    loads = [pltpu.make_async_copy(p_hbm, p_ref, load.at[0]), pltpu.make_async_copy(w_hbm, w_ref, load.at[1])]
    for copy in loads:
        copy.start()

    near = {(0,)} | {tuple(sorted({0, b} - {0} | extra)) for b in range(1, bits) for extra in ({0}, set())}
    for r in range(1, rounds):
        near.add(moves(r, bits))
    final = (rounds - 1) % bits
    across = {(), (0,), tuple({final} - {0}), tuple(sorted({0, final}))}
    peers = [(at, 0) for at in sorted(near | across) if at]
    peers += [(at, ds_) for ds_ in range(1, n_slab) for at in sorted(across)]
    barrier = pltpu.get_barrier_semaphore()
    for at, ds_ in peers:
        pl.semaphore_signal(barrier, inc=1, device_id=(flipped(*at), (slab + ds_) % n_slab),
                            device_id_type=pl.DeviceIdType.MESH)
    pl.semaphore_wait(barrier, len(peers))
    for copy in loads:
        copy.wait()

    def columns_of(slab_at, core_at):
        return pl.ds(pl.multiple_of((slab_at * 2 + core_at) * block, 128), block)

    base = slab * half
    rows_here = pl.ds(pl.multiple_of(base, half), half)
    gives, stills, moved = [], [], [[] for _ in parts[1:]]
    for ds_ in range(1, n_slab):
        gives.append(remote(w_ref.at[0, :, columns_of((slab + ds_) % n_slab, 1 - core)], stage.at[ds_ - 1],
                            give_send.at[ds_ - 1], give_recv.at[ds_ - 1], flipped(0), slab))
        gives[-1].start()
    own = pltpu.make_async_copy(w_ref.at[0, :, columns_of(slab, core)], init.at[odd, rows_here], first_recv.at[0])
    beside = remote(w_ref.at[0, :, columns_of(slab, 1 - core)], init.at[odd, rows_here], first_send,
                    first_recv.at[1], flipped(0), slab)

    def crossing(ds_, src, kind, k):
        slab_to = (slab + ds_) % n_slab
        if kind == 0:
            return remote(src, init.at[0, rows_here], still_send.at[ds_ - 1], still_recv.at[ds_ - 1], me, slab_to)
        size = parts[k + 1] - parts[k]
        dst = init.at[1, pl.ds(pl.multiple_of(base + parts[k], 16), size)]
        return remote(src.at[pl.ds(parts[k], size)], dst, in_send.at[ds_ - 1, k], in_recv.at[ds_ - 1, k], me, slab_to)

    def mine(ds_):
        return w_ref.at[0, :, columns_of((slab + ds_) % n_slab, core)]

    @pl.when(odd == 0)
    def _():
        for ds_ in range(1, n_slab):
            crossing(ds_, mine(ds_), 0, 0).start()

    own.start()
    beside.start()
    for copy in gives:
        copy.wait_recv()

    @pl.when(odd == 0)
    def _():
        for k in range(len(parts) - 1):
            for ds_ in range(1, n_slab):
                crossing(ds_, stage.at[ds_ - 1], 1, k).start()

    @pl.when(odd == 1)
    def _():
        for ds_ in range(1, n_slab):
            crossing(ds_, stage.at[ds_ - 1], 0, 0).start()
        for k in range(len(parts) - 1):
            for ds_ in range(1, n_slab):
                crossing(ds_, mine(ds_), 1, k).start()

    for ds_ in range(1, n_slab):
        stills.append(crossing(ds_, stage.at[ds_ - 1], 0, 0))
        for k in range(len(parts) - 1):
            moved[k].append(crossing(ds_, stage.at[ds_ - 1], 1, k))

    perms[0] = p_ref[0]
    for b in range(bits):
        for c in range(2):
            if 2 * b + c > 0:
                to = flipped(b) if c == 0 else (flipped(0, b) if b else flipped(0))
                remote(p_ref.at[0], perms.at[2 * b + c], perm_send, perm_recv, to, slab).start()
    others = perms.at[pl.ds(1, 2 * bits - 1)]
    spread_all = remote(others, others, perm_send, perm_recv, flipped(0), slab)

    def visitor_of(r):
        return init.at[1] if r == 0 else vis.at[r - 1]

    def merged(own, mix, other):
        aligned = 0.5 * jnp.dot(mix, other, preferred_element_type=jnp.float32)
        return ((own.astype(jnp.float32) + aligned) * (1.0 / math.sqrt(2.0))).astype(jnp.bfloat16)

    chunks = [pl.ds(k * CHUNK, CHUNK) for k in range(block // CHUNK)]
    cuts = [(h * half + a, h * half + b) for a, b in zip(parts[:-1], parts[1:]) for h in range(n_slab)]
    spans = [pl.ds(a, b - a) for a, b in cuts]
    columns = lax.broadcasted_iota(jnp.int32, (ffw, ffw), 1)
    rows = lax.broadcasted_iota(jnp.int32, (ffw, ffw), 0)

    spread_all.wait()
    for r in range(rounds):
        b = r % bits
        rows_v[r:r + 1, :] = (perms[2 * b + odd, r:r + 1, :] if b else perms[1 - odd, r:r + 1, :]).astype(jnp.float32)
    cols_v[...] = rows_v[...].T
    for r in range(rounds):
        hot_v[r] = (cols_v[:, r:r + 1].astype(jnp.int32) == columns).astype(jnp.float32)
        hot_r[r] = (perms[odd, r:r + 1, :] == rows).astype(jnp.float32)
    own.wait()
    beside.wait_recv()
    for copy in stills:
        copy.wait_recv()

    pending = gives + [beside] + stills + sum(moved, [])
    arrivals = None
    source = slab * 2 + core
    for r in range(rounds):
        last = r == rounds - 1
        visitor = visitor_of(r)
        sums = [[] for _ in spans]
        total_columns = [None]
        onward = []

        def cost(q):
            its = spans[q]
            if r:
                arrivals[q].wait_recv()
            elif q % n_slab == 0:
                for copy in moved[q // n_slab]:
                    copy.wait_recv()
            partial = lax.dot_general(visitor[its, :], init[0], (((1,), (1,)), ((), ())),
                                      preferred_element_type=jnp.float32)
            part[r, its, :] = partial
            half_out[r, its, :] = partial.astype(half_out.dtype)
            for ds_ in range(1, n_slab):
                for dc in range(2):
                    at = 2 * (ds_ - 1) + dc
                    sums[q].append(remote(half_out.at[r, its], half_in.at[r, at, its], half_send.at[r, at, q],
                                          half_recv.at[r, at, q], me if dc == 0 else flipped(0),
                                          (slab + ds_) % n_slab))
            sums[q].append(remote(part.at[r, its], core_in.at[r, its], core_send.at[r, q], core_recv.at[r, q],
                                  flipped(0), slab))
            for copy in sums[q]:
                copy.start()

        def finish(q):
            its = spans[q]
            for copy in sums[q]:
                copy.wait_recv()
            total = part[r, its, :] + core_in[r, its, :]
            for at in range(2 * (n_slab - 1)):
                total = total + half_in[r, at, its, :].astype(jnp.float32)
            scaled = total * scale
            squared = scaled * scaled
            fourth = squared * squared
            fourths[its, :] = fourth
            by_row = 1.0 / (1.0 + jnp.sum(fourth, axis=1, keepdims=True))
            mix = (hot_v[r, its, :] + fourth * by_row).astype(jnp.bfloat16)
            for k in chunks:
                sent[r, its, k] = merged(visitor[its, k], mix, init[0, :, k])
            if last:
                h = cuts[q][0] // half
                dst = out_ref.at[0, pl.ds(cuts[q][0] - h * half, cuts[q][1] - cuts[q][0]),
                                 pl.ds(pl.multiple_of(source * block, 128), block)]
                j = resident_flipped(r % bits)
                copy = remote(sent.at[r, its], dst, out_send.at[q], out_recv.at[source], j, h)
            else:
                copy = remote(sent.at[r, its], vis.at[r, its], ex_send.at[r, q], ex_recv.at[r, q],
                              flipped(*moves(r + 1, bits)), slab)
            copy.start()
            onward.append(copy)
            by_columns = jnp.sum(fourth, axis=0, keepdims=True)
            total_columns[0] = by_columns if total_columns[0] is None else total_columns[0] + by_columns

        def resident_flipped(b):
            if b == 0:
                return me + (1 - odd) * (1 - 2 * core)
            return resident + (1 - 2 * bit(b)) * (1 << b)

        lag = len(spans) if r == 0 else 1 if r % bits and bits - 1 in moves(r, bits) + moves(r + 1, bits) else LAG
        for q in range(len(spans) + lag):
            if q < len(spans):
                cost(q)
            if q >= lag:
                finish(q - lag)

        by_column = 1.0 / (1.0 + total_columns[0])
        mix = (hot_r[r] + fourths[...] * by_column).astype(jnp.bfloat16).T
        for k in chunks:
            init[0, :, k] = merged(init[0, :, k], mix, visitor[:, k])
        pending += sum(sums, [])
        arrivals = onward
        if last:
            for h in range(n_slab):
                src = init.at[0, pl.ds(h * half, half)]
                dst = out_ref.at[0, :, pl.ds(pl.multiple_of(source * block, 128), block)]
                stay = jnp.logical_and(odd == 0, slab == h)

                @pl.when(stay)
                def _():
                    pltpu.make_async_copy(src, dst, out_recv.at[source]).start()

                @pl.when(jnp.logical_not(stay))
                def _():
                    remote(src, dst, home_send.at[h], out_recv.at[source], resident, h).start()
            for copy in onward:
                copy.wait_send()
            for h in range(n_slab):
                stay = jnp.logical_and(odd == 0, slab == h)

                @pl.when(jnp.logical_not(stay))
                def _():
                    src = init.at[0, pl.ds(h * half, half)]
                    dst = out_ref.at[0, :, pl.ds(0, block)]
                    remote(src, dst, home_send.at[h], out_recv.at[0], resident, h).wait_send()
            for s in range(2 * n_slab):
                dst = out_ref.at[0, :, pl.ds(s * block, block)]
                pltpu.make_async_copy(dst, dst, out_recv.at[s]).wait()
        else:
            pending += onward
    for copy in pending:
        copy.wait_send()


def solution(mesh):
    n_rep, n_slab = mesh.shape["rep"], mesh.shape["slab"]

    def local(weights, perms):
        _, half, width = weights.shape
        rounds = perms.shape[1]
        ffw = perms.shape[2]
        bits = n_rep.bit_length() - 1
        block = width // (2 * n_slab)
        parts = [k * half // PARTS for k in range(PARTS + 1)]
        pieces = PARTS * n_slab
        vmem = pltpu.VMEM
        dma = pltpu.SemaphoreType.DMA
        bf16, f32 = jnp.bfloat16, jnp.float32
        away = 2 * (n_slab - 1)
        return pl.pallas_call(
            functools.partial(kernel, n_rep, n_slab, rounds, parts),
            out_shape=pltpu.VMEM(weights.shape, weights.dtype),
            in_specs=[pl.BlockSpec(memory_space=pl.ANY)] * 2,
            out_specs=pl.BlockSpec(memory_space=pltpu.VMEM),
            scratch_shapes=[
                vmem(weights.shape, bf16), vmem(perms.shape, jnp.int32),
                vmem((n_slab - 1, half, block), bf16),
                vmem((2, ffw, block), bf16),
                vmem((rounds - 1, ffw, block), bf16),
                vmem((rounds, ffw, block), bf16),
                vmem((rounds, ffw, ffw), f32),
                vmem((rounds, ffw, ffw), f32),
                vmem((rounds, ffw, ffw), bf16),
                vmem((rounds, away, ffw, ffw), bf16),
                vmem((ffw, ffw), f32),
                vmem((rounds, ffw, ffw), f32),
                vmem((rounds, ffw, ffw), f32),
                vmem((2 * bits, rounds, ffw), jnp.int32),
                vmem((rounds, ffw), f32),
                vmem((ffw, rounds), f32),
                dma((2,)), dma((n_slab - 1,)), dma((n_slab - 1,)), dma((n_slab - 1,)), dma((n_slab - 1,)),
                dma, dma((2,)), dma((n_slab - 1, PARTS)), dma((n_slab - 1, PARTS)),
                dma((rounds, pieces)), dma((rounds, pieces)),
                dma((rounds, pieces)), dma((rounds, pieces)),
                dma((rounds, away, pieces)), dma((rounds, away, pieces)),
                dma((pieces,)), dma((n_slab,)), dma((2 * n_slab,)),
                dma, dma,
            ],
            compiler_params=pltpu.CompilerParams(collective_id=0, has_side_effects=True, vmem_limit_bytes=60 * 1024 * 1024),
        )(weights, perms)

    return jax.shard_map(
        local, mesh=mesh, in_specs=(P("rep", "slab", None), P("rep", None, None)),
        out_specs=P("rep", "slab", None), check_vma=False,
    )
```

```python
import functools
import math

import jax
import jax.numpy as jnp
from jax import lax
from jax.experimental import pallas as pl
from jax.experimental.pallas import tpu as pltpu
from jax.sharding import PartitionSpec as P

CHUNK = 256
PARTS = 2
LAG = 2


def moves(r, bits):
    return tuple(sorted(b for b in ((r - 1) % bits, r % bits) if b))


def kernel(n_rep, n_slab, rounds, parts, w_hbm, p_hbm, out_ref,
           w_ref, p_ref, stage, init, vis, sent, part, core_in, half_out, half_in, fourths, hot_v, hot_r, perms, rows_v, cols_v,
           load, give_send, give_recv, still_send, still_recv, first_send, first_recv, in_send, in_recv, ex_send, ex_recv, core_send, core_recv, half_send, half_recv,
           out_send, home_send, out_recv, perm_send, perm_recv):
    bits = n_rep.bit_length() - 1
    me = lax.axis_index("rep")
    slab = lax.axis_index("slab")
    core = me % 2
    half, width = w_ref.shape[1], w_ref.shape[2]
    ffw = half * n_slab
    block = width // (2 * n_slab)
    scale = 1.0 / math.sqrt(width)

    def bit(b):
        return (me // (1 << b)) % 2

    def flipped(*at):
        to = me
        for b in at:
            to = to + (1 - 2 * bit(b)) * (1 << b)
        return to

    odd = sum(bit(b) for b in range(bits)) % 2
    resident = me + odd * (1 - 2 * core)

    def remote(src, dst, send, recv, rep_to, slab_to):
        return pltpu.make_async_remote_copy(
            src_ref=src, dst_ref=dst, send_sem=send, recv_sem=recv,
            device_id=(rep_to, slab_to), device_id_type=pl.DeviceIdType.MESH)

    loads = [pltpu.make_async_copy(p_hbm, p_ref, load.at[0]), pltpu.make_async_copy(w_hbm, w_ref, load.at[1])]
    for copy in loads:
        copy.start()

    near = {(0,)} | {tuple(sorted({0, b} - {0} | extra)) for b in range(1, bits) for extra in ({0}, set())}
    for r in range(1, rounds):
        near.add(moves(r, bits))
    final = (rounds - 1) % bits
    across = {(), (0,), tuple({final} - {0}), tuple(sorted({0, final}))}
    peers = [(at, 0) for at in sorted(near | across) if at]
    peers += [(at, ds_) for ds_ in range(1, n_slab) for at in sorted(across)]
    barrier = pltpu.get_barrier_semaphore()
    for at, ds_ in peers:
        pl.semaphore_signal(barrier, inc=1, device_id=(flipped(*at), (slab + ds_) % n_slab),
                            device_id_type=pl.DeviceIdType.MESH)
    pl.semaphore_wait(barrier, len(peers))
    for copy in loads:
        copy.wait()

    def columns_of(slab_at, core_at):
        return pl.ds(pl.multiple_of((slab_at * 2 + core_at) * block, 128), block)

    base = slab * half
    rows_here = pl.ds(pl.multiple_of(base, half), half)
    gives, stills, moved = [], [], [[] for _ in parts[1:]]
    for ds_ in range(1, n_slab):
        gives.append(remote(w_ref.at[0, :, columns_of((slab + ds_) % n_slab, 1 - core)], stage.at[ds_ - 1],
                            give_send.at[ds_ - 1], give_recv.at[ds_ - 1], flipped(0), slab))
        gives[-1].start()
    own = pltpu.make_async_copy(w_ref.at[0, :, columns_of(slab, core)], init.at[odd, rows_here], first_recv.at[0])
    beside = remote(w_ref.at[0, :, columns_of(slab, 1 - core)], init.at[odd, rows_here], first_send,
                    first_recv.at[1], flipped(0), slab)

    def crossing(ds_, src, kind, k):
        slab_to = (slab + ds_) % n_slab
        if kind == 0:
            return remote(src, init.at[0, rows_here], still_send.at[ds_ - 1], still_recv.at[ds_ - 1], me, slab_to)
        size = parts[k + 1] - parts[k]
        dst = init.at[1, pl.ds(pl.multiple_of(base + parts[k], 16), size)]
        return remote(src.at[pl.ds(parts[k], size)], dst, in_send.at[ds_ - 1, k], in_recv.at[ds_ - 1, k], me, slab_to)

    def mine(ds_):
        return w_ref.at[0, :, columns_of((slab + ds_) % n_slab, core)]

    @pl.when(odd == 0)
    def _():
        for ds_ in range(1, n_slab):
            crossing(ds_, mine(ds_), 0, 0).start()

    own.start()
    beside.start()
    for copy in gives:
        copy.wait_recv()

    @pl.when(odd == 0)
    def _():
        for k in range(len(parts) - 1):
            for ds_ in range(1, n_slab):
                crossing(ds_, stage.at[ds_ - 1], 1, k).start()

    @pl.when(odd == 1)
    def _():
        for ds_ in range(1, n_slab):
            crossing(ds_, stage.at[ds_ - 1], 0, 0).start()
        for k in range(len(parts) - 1):
            for ds_ in range(1, n_slab):
                crossing(ds_, mine(ds_), 1, k).start()

    for ds_ in range(1, n_slab):
        stills.append(crossing(ds_, stage.at[ds_ - 1], 0, 0))
        for k in range(len(parts) - 1):
            moved[k].append(crossing(ds_, stage.at[ds_ - 1], 1, k))

    perms[0] = p_ref[0]
    for b in range(bits):
        for c in range(2):
            if 2 * b + c > 0:
                to = flipped(b) if c == 0 else (flipped(0, b) if b else flipped(0))
                remote(p_ref.at[0], perms.at[2 * b + c], perm_send, perm_recv, to, slab).start()
    others = perms.at[pl.ds(1, 2 * bits - 1)]
    spread_all = remote(others, others, perm_send, perm_recv, flipped(0), slab)

    def visitor_of(r):
        return init.at[1] if r == 0 else vis.at[r - 1]

    def merged(own, mix, other):
        aligned = 0.5 * jnp.dot(mix, other, preferred_element_type=jnp.float32)
        return ((own.astype(jnp.float32) + aligned) * (1.0 / math.sqrt(2.0))).astype(jnp.bfloat16)

    chunks = [pl.ds(k * CHUNK, CHUNK) for k in range(block // CHUNK)]
    cuts = [(h * half + a, h * half + b) for a, b in zip(parts[:-1], parts[1:]) for h in range(n_slab)]
    spans = [pl.ds(a, b - a) for a, b in cuts]
    columns = lax.broadcasted_iota(jnp.int32, (ffw, ffw), 1)
    rows = lax.broadcasted_iota(jnp.int32, (ffw, ffw), 0)

    spread_all.wait()
    for r in range(rounds):
        b = r % bits
        rows_v[r:r + 1, :] = (perms[2 * b + odd, r:r + 1, :] if b else perms[1 - odd, r:r + 1, :]).astype(jnp.float32)
    cols_v[...] = rows_v[...].T
    for r in range(rounds):
        hot_v[r] = (cols_v[:, r:r + 1].astype(jnp.int32) == columns).astype(jnp.float32)
        hot_r[r] = (perms[odd, r:r + 1, :] == rows).astype(jnp.float32)
    own.wait()
    beside.wait_recv()
    for copy in stills:
        copy.wait_recv()

    pending = gives + [beside] + stills + sum(moved, [])
    arrivals = None
    source = slab * 2 + core
    for r in range(rounds):
        last = r == rounds - 1
        visitor = visitor_of(r)
        sums = [[] for _ in spans]
        total_columns = [None]
        onward = []

        def cost(q):
            its = spans[q]
            if r:
                arrivals[q].wait_recv()
            elif q % n_slab == 0:
                for copy in moved[q // n_slab]:
                    copy.wait_recv()
            partial = lax.dot_general(visitor[its, :], init[0], (((1,), (1,)), ((), ())),
                                      preferred_element_type=jnp.float32)
            part[r, its, :] = partial
            half_out[r, its, :] = partial.astype(half_out.dtype)
            for ds_ in range(1, n_slab):
                for dc in range(2):
                    at = 2 * (ds_ - 1) + dc
                    sums[q].append(remote(half_out.at[r, its], half_in.at[r, at, its], half_send,
                                          half_recv.at[r, q], me if dc == 0 else flipped(0),
                                          (slab + ds_) % n_slab))
            sums[q].append(remote(part.at[r, its], core_in.at[r, its], core_send, core_recv.at[r, q],
                                  flipped(0), slab))
            for copy in sums[q]:
                copy.start()

        def finish(q):
            its = spans[q]
            both = half_in.at[r, :, its]
            remote(both, both, half_send, half_recv.at[r, q], flipped(0), slab).wait_recv()
            sums[q][-1].wait_recv()
            total = part[r, its, :] + core_in[r, its, :]
            for at in range(2 * (n_slab - 1)):
                total = total + half_in[r, at, its, :].astype(jnp.float32)
            scaled = total * scale
            squared = scaled * scaled
            fourth = squared * squared
            fourths[its, :] = fourth
            by_row = 1.0 / (1.0 + jnp.sum(fourth, axis=1, keepdims=True))
            mix = (hot_v[r, its, :] + fourth * by_row).astype(jnp.bfloat16)
            for k in chunks:
                sent[r, its, k] = merged(visitor[its, k], mix, init[0, :, k])
            if last:
                h = cuts[q][0] // half
                dst = out_ref.at[0, pl.ds(cuts[q][0] - h * half, cuts[q][1] - cuts[q][0]),
                                 pl.ds(pl.multiple_of(source * block, 128), block)]
                j = resident_flipped(r % bits)
                copy = remote(sent.at[r, its], dst, out_send, out_recv.at[source], j, h)
            else:
                copy = remote(sent.at[r, its], vis.at[r, its], ex_send, ex_recv.at[r, q],
                              flipped(*moves(r + 1, bits)), slab)
            copy.start()
            onward.append(copy)
            by_columns = jnp.sum(fourth, axis=0, keepdims=True)
            total_columns[0] = by_columns if total_columns[0] is None else total_columns[0] + by_columns

        def resident_flipped(b):
            if b == 0:
                return me + (1 - odd) * (1 - 2 * core)
            return resident + (1 - 2 * bit(b)) * (1 << b)

        lag = len(spans) if r == 0 else 1 if r % bits and bits - 1 in moves(r, bits) + moves(r + 1, bits) else LAG
        for q in range(len(spans) + lag):
            if q < len(spans):
                cost(q)
            if q >= lag:
                finish(q - lag)

        by_column = 1.0 / (1.0 + total_columns[0])
        mix = (hot_r[r] + fourths[...] * by_column).astype(jnp.bfloat16).T
        for k in chunks:
            init[0, :, k] = merged(init[0, :, k], mix, visitor[:, k])
        arrivals = onward
        if last:
            for h in range(n_slab):
                src = init.at[0, pl.ds(h * half, half)]
                dst = out_ref.at[0, :, pl.ds(pl.multiple_of(source * block, 128), block)]
                stay = jnp.logical_and(odd == 0, slab == h)

                @pl.when(stay)
                def _():
                    pltpu.make_async_copy(src, dst, out_recv.at[source]).start()

                @pl.when(jnp.logical_not(stay))
                def _():
                    remote(src, dst, home_send.at[h], out_recv.at[source], resident, h).start()
            for copy in pending:
                copy.wait_send()
            for whole, sem in ((half_in, half_send), (core_in, core_send), (vis, ex_send), (sent.at[r], out_send)):
                remote(whole, whole, sem, out_recv.at[0], flipped(0), slab).wait_send()
            for h in range(n_slab):
                stay = jnp.logical_and(odd == 0, slab == h)

                @pl.when(jnp.logical_not(stay))
                def _():
                    src = init.at[0, pl.ds(h * half, half)]
                    dst = out_ref.at[0, :, pl.ds(0, block)]
                    remote(src, dst, home_send.at[h], out_recv.at[0], resident, h).wait_send()
            for s in range(2 * n_slab):
                dst = out_ref.at[0, :, pl.ds(s * block, block)]
                pltpu.make_async_copy(dst, dst, out_recv.at[s]).wait()


def solution(mesh):
    n_rep, n_slab = mesh.shape["rep"], mesh.shape["slab"]

    def local(weights, perms):
        _, half, width = weights.shape
        rounds = perms.shape[1]
        ffw = perms.shape[2]
        bits = n_rep.bit_length() - 1
        block = width // (2 * n_slab)
        parts = [k * half // PARTS for k in range(PARTS + 1)]
        pieces = PARTS * n_slab
        vmem = pltpu.VMEM
        dma = pltpu.SemaphoreType.DMA
        bf16, f32 = jnp.bfloat16, jnp.float32
        away = 2 * (n_slab - 1)
        return pl.pallas_call(
            functools.partial(kernel, n_rep, n_slab, rounds, parts),
            out_shape=pltpu.VMEM(weights.shape, weights.dtype),
            in_specs=[pl.BlockSpec(memory_space=pl.ANY)] * 2,
            out_specs=pl.BlockSpec(memory_space=pltpu.VMEM),
            scratch_shapes=[
                vmem(weights.shape, bf16), vmem(perms.shape, jnp.int32),
                vmem((n_slab - 1, half, block), bf16),
                vmem((2, ffw, block), bf16),
                vmem((rounds - 1, ffw, block), bf16),
                vmem((rounds, ffw, block), bf16),
                vmem((rounds, ffw, ffw), f32),
                vmem((rounds, ffw, ffw), f32),
                vmem((rounds, ffw, ffw), bf16),
                vmem((rounds, away, ffw, ffw), bf16),
                vmem((ffw, ffw), f32),
                vmem((rounds, ffw, ffw), f32),
                vmem((rounds, ffw, ffw), f32),
                vmem((2 * bits, rounds, ffw), jnp.int32),
                vmem((rounds, ffw), f32),
                vmem((ffw, rounds), f32),
                dma((2,)), dma((n_slab - 1,)), dma((n_slab - 1,)), dma((n_slab - 1,)), dma((n_slab - 1,)),
                dma, dma((2,)), dma((n_slab - 1, PARTS)), dma((n_slab - 1, PARTS)),
                dma, dma((rounds - 1, pieces)),
                dma, dma((rounds, pieces)),
                dma, dma((rounds, pieces)),
                dma, dma((n_slab,)), dma((2 * n_slab,)),
                dma, dma,
            ],
            compiler_params=pltpu.CompilerParams(collective_id=0, has_side_effects=True, vmem_limit_bytes=60 * 1024 * 1024),
        )(weights, perms)

    return jax.shard_map(
        local, mesh=mesh, in_specs=(P("rep", "slab", None), P("rep", None, None)),
        out_specs=P("rep", "slab", None), check_vma=False,
    )
```
